8 devices in a mesh: dp: 1 (over z), sp: 8 (over x, y, core).
Axes of the slice: x: 2, y: 2, z: 1, core: 2. Of those that a mesh axis runs over, the one named last changes fastest.
Arguments:
- q: bfloat16 [32, 56, 128], P('dp')
- k: bfloat16 [32, 2048, 56, 128], P('dp', 'sp')
- v: bfloat16 [32, 2048, 56, 128], P('dp', 'sp')
Outputs:
- q: bfloat16 [32, 56, 128], P('dp')
All inputs are finite; a program needn't handle non-finite values.
Results may differ from the reference program's by a relative error of at most 0.012.
Values are sent between devices in bfloat16 or wider.
A program may use at most 2 GiB of HBM per device.

```python
import jax
import jax.numpy as jnp

BATCH = 32
CACHE = 2048
HEADS = 56
KV_HEADS = 56
HEAD = 128


def setup_inputs(seed: int = 0, part: int = 0) -> dict:
    kq, kk, kv = (jax.random.fold_in(k, part) for k in jax.random.split(jax.random.key(seed), 3))
    return {
        "q": (3 * jax.random.normal(kq, (BATCH, HEADS, HEAD), jnp.float32)).astype(jnp.bfloat16),
        "k": jax.random.normal(kk, (BATCH, CACHE, KV_HEADS, HEAD), jnp.float32).astype(jnp.bfloat16),
        "v": jax.random.normal(kv, (BATCH, CACHE, KV_HEADS, HEAD), jnp.float32).astype(jnp.bfloat16),
    }


def einsum(form, a, b):
    return jnp.einsum(form, a.astype(jnp.float32), b.astype(jnp.float32))


def reference(q, k, v):
    grouped = q.reshape(BATCH, KV_HEADS, -1, HEAD)
    scores = einsum("bgsd,bugd->bgsu", grouped, k) * HEAD**-0.5
    weights = jax.nn.softmax(scores, -1).astype(jnp.bfloat16)
    return einsum("bgsu,bugd->bgsd", weights, v).astype(jnp.bfloat16).reshape(BATCH, HEADS, HEAD)
```

```python
import functools

import jax
import jax.numpy as jnp
from jax import lax
from jax.experimental import pallas as pl
from jax.experimental.pallas import tpu as pltpu
from jax.sharding import PartitionSpec as P

MESH = pl.DeviceIdType.MESH
LOG2E = 1.4426950408889634
SLOTS = 4
LAG = 4
ROWS = 16


def kernel(n, q_hbm, k_hbm, v_hbm, o_hbm, kbuf, vbuf, qbuf, part, stat, out, ksem, vsem, qsem, osem, send_sem, recv_sem):
    batch, pairs, groups, rows, head = k_hbm.shape
    heads = q_hbm.shape[1]
    half = pairs // 2
    tiles = heads // 8
    me = lax.axis_index("sp")
    dp = lax.axis_index("dp")
    scale = head**-0.5 * LOG2E

    def fetch(b, slot):
        return (
            pltpu.make_async_copy(k_hbm.at[b], kbuf.at[slot], ksem.at[slot]),
            pltpu.make_async_copy(v_hbm.at[b], vbuf.at[slot], vsem.at[slot]),
        )

    q_copy = pltpu.make_async_copy(q_hbm, qbuf, qsem)
    q_copy.start()
    for slot in range(SLOTS):
        for copy in fetch(slot, slot):
            copy.start()

    barrier = pltpu.get_barrier_semaphore()
    for i in range(1, n):
        pl.semaphore_signal(barrier, inc=1, device_id=(dp, lax.rem(me + i, n)), device_id_type=MESH)
    q_copy.wait()
    pl.semaphore_wait(barrier, n - 1)

    def sends(b, i):
        peer = (dp, lax.rem(me + i, n))
        return [
            pltpu.make_async_remote_copy(
                src_ref=ref.at[me, b],
                dst_ref=ref.at[me, b],
                send_sem=send_sem.at[x],
                recv_sem=recv_sem.at[x, b],
                device_id=peer,
                device_id_type=MESH,
            )
            for x, ref in enumerate((part, stat))
        ]

    def attend(b, slot):
        q32 = qbuf[b].astype(jnp.float32)
        qq = jnp.concatenate([q32, q32], 0)
        row = lax.broadcasted_iota(jnp.int32, (2 * ROWS, half * ROWS), 0) % ROWS
        col = lax.broadcasted_iota(jnp.int32, (2 * ROWS, half * ROWS), 1) % ROWS
        own = row == col
        zero = jnp.zeros((ROWS, head), jnp.bfloat16)
        sums, highs, totals = [], [], []
        for j in range(groups):
            q16 = qq[ROWS * j : ROWS * (j + 1)].astype(jnp.bfloat16)
            lhs = jnp.concatenate([jnp.concatenate([q16, zero], 1), jnp.concatenate([zero, q16], 1)], 0)
            keys = [kbuf[slot, half * a : half * (a + 1), j].reshape(half * ROWS, head) for a in range(2)]
            s = lax.dot_general(
                lhs, jnp.concatenate(keys, 1), (((1,), (1,)), ((), ())), preferred_element_type=jnp.float32
            )
            s = jnp.where(own, s, -jnp.inf)
            high = jnp.max(s, 1, keepdims=True)
            high = jnp.maximum(high[:ROWS], high[ROWS:])
            p = jnp.exp2((s - jnp.concatenate([high, high], 0)) * scale)
            total = jnp.sum(p, 1, keepdims=True)
            values = [vbuf[slot, half * a : half * (a + 1), j].reshape(half * ROWS, head) for a in range(2)]
            o = jnp.dot(p.astype(jnp.bfloat16), jnp.concatenate(values, 1), preferred_element_type=jnp.float32)
            o = o[:ROWS, :head] + o[ROWS:, head:]
            total = total[:ROWS] + total[ROWS:]
            for t in range(ROWS // 8):
                rows8 = slice(8 * t, 8 * (t + 1))
                sums.append(o[rows8])
                highs.append(high[rows8])
                totals.append(total[rows8])
        lane = lax.broadcasted_iota(jnp.int32, (8, head), 1)
        tile = jnp.zeros((8, head), jnp.float32)
        seen = []
        for g in range(tiles):
            high = jnp.maximum(highs[g], highs[g + tiles])
            e0 = jnp.exp2((highs[g] - high) * scale)
            e1 = jnp.exp2((highs[g + tiles] - high) * scale)
            seen.append(sums[g] * e0 + sums[g + tiles] * e1)
            tile = jnp.where(lane == g, high, tile)
            tile = jnp.where(lane == g + 8, totals[g] * e0 + totals[g + tiles] * e1, tile)
        part[me, b] = jnp.concatenate(seen, 0).astype(jnp.bfloat16)
        stat[me, b] = tile

    def together(b):
        for x, ref in enumerate((part, stat)):
            peers = ref.at[pl.ds(0, n - 1), b]
            pltpu.make_async_copy(peers, peers, recv_sem.at[x, b]).wait()
        stats = [stat[i, b] for i in range(n)]
        high = functools.reduce(jnp.maximum, stats)
        weights = [jnp.exp2((s - high) * scale) for s in stats]
        total = sum(w * pltpu.roll(s, head - 8, 1) for w, s in zip(weights, stats))
        weights = [w / total for w in weights]
        acc = [jnp.zeros((8, head), jnp.float32)] * tiles
        for i in range(n):
            mine = part[i, b].astype(jnp.float32)
            for g in range(tiles):
                acc[g] = acc[g] + mine[8 * g : 8 * (g + 1)] * weights[i][:, g : g + 1]
        out[b] = jnp.concatenate(acc, 0).astype(jnp.bfloat16)
        pltpu.make_async_copy(out.at[b], o_hbm.at[b], osem).start()

    def step(b, _):
        slot = lax.rem(b, SLOTS)
        for copy in fetch(b, slot):
            copy.wait()
        attend(b, slot)
        for i in range(1, n):
            for copy in sends(b, i):
                copy.start()

        @pl.when(b + SLOTS < batch)
        def _():
            for copy in fetch(b + SLOTS, slot):
                copy.start()

        @pl.when(b >= LAG)
        def _():
            together(b - LAG)

        return 0

    lax.fori_loop(0, batch, step, 0)
    lax.fori_loop(batch - LAG, batch, lambda b, _: (together(b), 0)[1], 0)

    for x, ref in enumerate((part, stat)):
        peers = ref.at[pl.ds(0, n - 1)]
        pltpu.make_async_copy(peers, peers, send_sem.at[x]).wait()
    pltpu.make_async_copy(out, o_hbm, osem).wait()


def solution(mesh):
    n = mesh.shape["sp"]

    def step(q, k, v):
        batch, heads, head = q.shape
        tokens = k.shape[1]
        groups = 2 * heads // ROWS
        shape = (batch, tokens // 2, groups, ROWS, head)
        return pl.pallas_call(
            functools.partial(kernel, n),
            out_shape=jax.ShapeDtypeStruct(q.shape, q.dtype),
            in_specs=[pl.BlockSpec(memory_space=pl.ANY)] * 3,
            out_specs=pl.BlockSpec(memory_space=pl.ANY),
            scratch_shapes=[
                pltpu.VMEM((SLOTS,) + shape[1:], jnp.bfloat16),
                pltpu.VMEM((SLOTS,) + shape[1:], jnp.bfloat16),
                pltpu.VMEM(q.shape, jnp.bfloat16),
                pltpu.VMEM((n, batch, heads, head), jnp.bfloat16),
                pltpu.VMEM((n, batch, 8, head), jnp.float32),
                pltpu.VMEM(q.shape, jnp.bfloat16),
                pltpu.SemaphoreType.DMA((SLOTS,)),
                pltpu.SemaphoreType.DMA((SLOTS,)),
                pltpu.SemaphoreType.DMA,
                pltpu.SemaphoreType.DMA,
                pltpu.SemaphoreType.DMA((2,)),
                pltpu.SemaphoreType.DMA((2, batch)),
            ],
            compiler_params=pltpu.CompilerParams(
                collective_id=0, has_side_effects=True, vmem_limit_bytes=60 * 1024 * 1024
            ),
        )(q, k.reshape(shape), v.reshape(shape))

    return jax.shard_map(
        step,
        mesh=mesh,
        in_specs=(P("dp", None, None), P("dp", "sp", None, None), P("dp", "sp", None, None)),
        out_specs=P("dp", None, None),
        check_vma=False,
    )
```

```python
import functools

import jax
import jax.numpy as jnp
from jax import lax
from jax.experimental import pallas as pl
from jax.experimental.pallas import tpu as pltpu
from jax.sharding import PartitionSpec as P

MESH = pl.DeviceIdType.MESH
LOG2E = 1.4426950408889634
SLOTS = 4
LAG = 3
ROWS = 16
TILE = 256
DELAY = 5


def kernel(
    n, q_hbm, k_hbm, v_hbm, o_hbm, kbuf, vbuf, qbuf, part, stat, part_in, stat_in, out,
    ksem, vsem, qsem, osem, done_sem, send_sem, recv_sem
):
    batch, half, _, groups, _, head = k_hbm.shape
    heads = q_hbm.shape[1]
    tiles = heads // 8
    me = lax.axis_index("sp")
    dp = lax.axis_index("dp")
    scale = head**-0.5 * LOG2E

    def fetch_k(b):
        slot = lax.rem(b, SLOTS)
        return pltpu.make_async_copy(k_hbm.at[b], kbuf.at[slot], ksem.at[slot])

    def fetch_v(b):
        slot = lax.rem(b, SLOTS)
        return pltpu.make_async_copy(v_hbm.at[b], vbuf.at[slot], vsem.at[slot])

    q_copy = pltpu.make_async_copy(q_hbm, qbuf, qsem)
    q_copy.start()
    for b in range(SLOTS):
        fetch_k(b).start()
        fetch_v(b).start()

    barrier = pltpu.get_barrier_semaphore()
    for i in range(1, n):
        pl.semaphore_signal(barrier, inc=1, device_id=(dp, lax.rem(me + i, n)), device_id_type=MESH)
    q_copy.wait()
    pl.semaphore_wait(barrier, n - 1)

    owned = batch - batch % n - n
    rounds = owned // n

    def seat(b):
        return jnp.where(b < owned, b // n, b - owned + rounds)

    def give(b, peer):
        for x, (ref, dst) in enumerate(((part, part_in), (stat, stat_in))):
            pltpu.make_async_remote_copy(
                src_ref=ref.at[b],
                dst_ref=dst.at[me, seat(b)],
                send_sem=send_sem.at[x],
                recv_sem=recv_sem.at[x, seat(b)],
                device_id=(dp, peer),
                device_id_type=MESH,
            ).start()

    def send(b):
        @pl.when((b < owned) & (lax.rem(b, n) != me))
        def _():
            give(b, lax.rem(b, n))

        @pl.when(b >= owned)
        def _():
            for i in range(1, n):
                give(b, lax.rem(me + i, n))

    def spread(b):
        for i in range(1, n):
            pltpu.make_async_remote_copy(
                src_ref=out.at[b],
                dst_ref=out.at[b],
                send_sem=send_sem.at[2],
                recv_sem=done_sem,
                device_id=(dp, lax.rem(me + i, n)),
                device_id_type=MESH,
            ).start()

    def finish(b):
        @pl.when((b >= owned) | (lax.rem(b, n) == me))
        def _():
            together(b)

        @pl.when((b < owned) & (lax.rem(b, n) == me))
        def _():
            spread(b)

    tiles_in = half * ROWS // TILE

    def tile_of(buf, slot, j, t):
        step = TILE // ROWS
        rows = [buf[slot, step * t : step * (t + 1), a, j].reshape(TILE, head) for a in range(2)]
        return jnp.concatenate(rows, 1)

    def eight(pieces, g):
        return pieces[8 * g // ROWS][8 * g % ROWS : 8 * g % ROWS + 8]

    def attend(b):
        q32 = qbuf[b].astype(jnp.float32)
        qq = jnp.concatenate([q32, q32], 0)
        row = lax.broadcasted_iota(jnp.int32, (2 * ROWS, TILE), 0) % ROWS
        col = lax.broadcasted_iota(jnp.int32, (2 * ROWS, TILE), 1) % ROWS
        own = row == col
        zero = jnp.zeros((ROWS, head), jnp.bfloat16)
        slot = lax.rem(b, SLOTS)
        pieces = range(tiles_in)
        sums, highs, totals, weights = {}, {}, {}, {}

        def score(j):
            q16 = qq[ROWS * j : ROWS * (j + 1)].astype(jnp.bfloat16)
            lhs = jnp.concatenate([jnp.concatenate([q16, zero], 1), jnp.concatenate([zero, q16], 1)], 0)
            s = {}
            for t in pieces:
                rhs = tile_of(kbuf, slot, j, t)
                s[t] = lax.dot_general(lhs, rhs, (((1,), (1,)), ((), ())), preferred_element_type=jnp.float32)
                s[t] = jnp.where(own, s[t], -jnp.inf)
            high = jnp.max(functools.reduce(jnp.maximum, s.values()), 1, keepdims=True)
            high = jnp.maximum(high[:ROWS], high[ROWS:])
            both = jnp.concatenate([high, high], 0)
            p = {t: jnp.exp2((s[t] - both) * scale) for t in s}
            total = jnp.sum(sum(p.values()), 1, keepdims=True)
            weights[j] = {t: p[t].astype(jnp.bfloat16) for t in p}
            highs[j], totals[j] = high, total[:ROWS] + total[ROWS:]

        def value(j):
            o = sum(
                jnp.dot(weights[j][t], tile_of(vbuf, slot, j, t), preferred_element_type=jnp.float32) for t in pieces
            )
            sums[j] = o[:ROWS, :head] + o[ROWS:, head:]

        for j in range(groups + DELAY):
            if j < groups:
                score(j)
            if j >= DELAY:
                value(j - DELAY)
        lane = lax.broadcasted_iota(jnp.int32, (8, head), 1)
        tile = jnp.zeros((8, head), jnp.float32)
        seen = []
        for g in range(tiles):
            h0, h1 = eight(highs, g), eight(highs, g + tiles)
            high = jnp.maximum(h0, h1)
            e0 = jnp.exp2((h0 - high) * scale)
            e1 = jnp.exp2((h1 - high) * scale)
            seen.append(eight(sums, g) * e0 + eight(sums, g + tiles) * e1)
            tile = jnp.where(lane == g, high, tile)
            tile = jnp.where(lane == g + 8, eight(totals, g) * e0 + eight(totals, g + tiles) * e1, tile)
        part[b] = jnp.concatenate(seen, 0).astype(jnp.bfloat16)
        stat[b] = tile

    def together(b):
        for x, ref in enumerate((part_in, stat_in)):
            peers = ref.at[pl.ds(0, n - 1), seat(b)]
            pltpu.make_async_copy(peers, peers, recv_sem.at[x, seat(b)]).wait()
        others = [lax.rem(me + i, n) for i in range(1, n)]
        stats = [stat[b]] + [stat_in[i, seat(b)] for i in others]
        high = functools.reduce(jnp.maximum, stats)
        weights = [jnp.exp2((s - high) * scale) for s in stats]
        total = sum(w * pltpu.roll(s, head - 8, 1) for w, s in zip(weights, stats))
        weights = [w / total for w in weights]
        acc = [jnp.zeros((8, head), jnp.float32)] * tiles
        for i in range(n):
            mine = (part_in[others[i - 1], seat(b)] if i else part[b]).astype(jnp.float32)
            for g in range(tiles):
                acc[g] = acc[g] + mine[8 * g : 8 * (g + 1)] * weights[i][:, g : g + 1]
        out[b] = jnp.concatenate(acc, 0).astype(jnp.bfloat16)

    def step(b, _):
        fetch_k(b).wait()
        fetch_v(b).wait()
        attend(b)
        send(b)

        @pl.when(b + SLOTS < batch)
        def _():
            fetch_k(b + SLOTS).start()
            fetch_v(b + SLOTS).start()

        @pl.when(b >= LAG)
        def _():
            finish(b - LAG)

        return 0

    lax.fori_loop(0, batch, step, 0)
    lax.fori_loop(batch - LAG, batch, lambda b, _: (finish(b), 0)[1], 0)
    for x, ref in enumerate((part_in, stat_in)):
        sent = ref.at[pl.ds(0, n - 1), pl.ds(0, rounds + n)]
        pltpu.make_async_copy(sent, sent, send_sem.at[x]).wait()
    sent = out.at[pl.ds(0, (n - 1) * rounds)]
    pltpu.make_async_copy(sent, sent, send_sem.at[2]).wait()
    pltpu.make_async_copy(sent, sent, done_sem).wait()
    copy = pltpu.make_async_copy(out, o_hbm, osem)
    copy.start()
    copy.wait()


def solution(mesh):
    n = mesh.shape["sp"]

    def step(q, k, v):
        batch, heads, head = q.shape
        tokens = k.shape[1]
        groups = 2 * heads // ROWS
        seats = batch // n - 1 + n
        shape = (batch, tokens // 4, 2, groups, ROWS, head)
        return pl.pallas_call(
            functools.partial(kernel, n),
            out_shape=jax.ShapeDtypeStruct(q.shape, q.dtype),
            in_specs=[pl.BlockSpec(memory_space=pl.ANY)] * 3,
            out_specs=pl.BlockSpec(memory_space=pl.ANY),
            scratch_shapes=[
                pltpu.VMEM((SLOTS,) + shape[1:], jnp.bfloat16),
                pltpu.VMEM((SLOTS,) + shape[1:], jnp.bfloat16),
                pltpu.VMEM(q.shape, jnp.bfloat16),
                pltpu.VMEM(q.shape, jnp.bfloat16),
                pltpu.VMEM((batch, 8, head), jnp.float32),
                pltpu.VMEM((n, seats, heads, head), jnp.bfloat16),
                pltpu.VMEM((n, seats, 8, head), jnp.float32),
                pltpu.VMEM(q.shape, jnp.bfloat16),
                pltpu.SemaphoreType.DMA((SLOTS,)),
                pltpu.SemaphoreType.DMA((SLOTS,)),
                pltpu.SemaphoreType.DMA,
                pltpu.SemaphoreType.DMA,
                pltpu.SemaphoreType.DMA,
                pltpu.SemaphoreType.DMA((3,)),
                pltpu.SemaphoreType.DMA((2, seats)),
            ],
            compiler_params=pltpu.CompilerParams(
                collective_id=0, has_side_effects=True, vmem_limit_bytes=60 * 1024 * 1024
            ),
        )(q, k.reshape(shape), v.reshape(shape))

    return jax.shard_map(
        step,
        mesh=mesh,
        in_specs=(P("dp", None, None), P("dp", "sp", None, None), P("dp", "sp", None, None)),
        out_specs=P("dp", None, None),
        check_vma=False,
    )
```

```python
import functools

import jax
import jax.numpy as jnp
from jax import lax
from jax.experimental import pallas as pl
from jax.experimental.pallas import tpu as pltpu
from jax.sharding import PartitionSpec as P

MESH = pl.DeviceIdType.MESH
LOG2E = 1.4426950408889634
LAG = 2
KEY_SLOTS = 4
VALUE_SLOTS = 3
TAIL = 2
ROWS = 16
TILE = 256
DELAY = 5


def kernel(
    n, q_hbm, k_hbm, v_hbm, out, kbuf, vbuf, qbuf, part, stat, part_in, stat_in,
    ksem, vsem, qsem, done_sem, spread_sem, give_sem, send_sem, recv_sem
):
    batch, half, _, groups, _, head = k_hbm.shape
    heads = q_hbm.shape[1]
    tiles = heads // 8
    me = lax.axis_index("sp")
    dp = lax.axis_index("dp")
    scale = head**-0.5 * LOG2E

    def fetch(hbm, buf, sem, b):
        slot = lax.rem(b, buf.shape[0])
        return pltpu.make_async_copy(hbm.at[b], buf.at[slot], sem.at[slot])

    def key_copy(b):
        return fetch(k_hbm, kbuf, ksem, b)

    def value_copy(b):
        return fetch(v_hbm, vbuf, vsem, b)

    q_copy = pltpu.make_async_copy(q_hbm, qbuf, qsem)
    q_copy.start()
    key_copy(0).start()
    value_copy(0).start()

    barrier = pltpu.get_barrier_semaphore()
    for i in range(1, n):
        pl.semaphore_signal(barrier, inc=1, device_id=(dp, lax.rem(me + i, n)), device_id_type=MESH)
    q_copy.wait()
    key_copy(1).start()
    value_copy(1).start()
    key_copy(2).start()
    pl.semaphore_wait(barrier, n - 1)

    owned = batch - TAIL
    rounds = -(-owned // n)

    def seat(b):
        return jnp.where(b < owned, b // n, b - owned + rounds)

    def give(x, b, peer, sem):
        ref, dst = ((part, part_in), (stat, stat_in))[x]
        pltpu.make_async_remote_copy(
            src_ref=ref.at[b],
            dst_ref=dst.at[me, seat(b)],
            send_sem=sem,
            recv_sem=recv_sem.at[x, seat(b)],
            device_id=(dp, peer),
            device_id_type=MESH,
        ).start()

    def give_owner(b):
        @pl.when(lax.rem(b, n) != me)
        def _():
            for x in range(2):
                give(x, b, lax.rem(b, n), give_sem.at[x, b])

    def give_all(x, b):
        for i in reversed(range(1, n)):
            give(x, b, lax.rem(me + i, n), send_sem.at[x])

    def spread(b):
        for i in range(1, n):
            pltpu.make_async_remote_copy(
                src_ref=out.at[b],
                dst_ref=out.at[b],
                send_sem=spread_sem.at[b],
                recv_sem=done_sem.at[b],
                device_id=(dp, lax.rem(me + i, n)),
                device_id_type=MESH,
            ).start()

    def finish(b):
        @pl.when(lax.rem(b, n) == me)
        def _():
            together(b)
            spread(b)

    tiles_in = half * ROWS // TILE

    def tile_of(buf, slot, j, t):
        step = TILE // ROWS
        rows = [buf[slot, step * t : step * (t + 1), a, j].reshape(TILE, head) for a in range(2)]
        return jnp.concatenate(rows, 1)

    def eight(pieces, g):
        return pieces[8 * g // ROWS][8 * g % ROWS : 8 * g % ROWS + 8]

    def attend(b, delay, between=None):
        q32 = qbuf[b].astype(jnp.float32)
        qq = jnp.concatenate([q32, q32], 0)
        row = lax.broadcasted_iota(jnp.int32, (2 * ROWS, TILE), 0) % ROWS
        col = lax.broadcasted_iota(jnp.int32, (2 * ROWS, TILE), 1) % ROWS
        own = row == col
        zero = jnp.zeros((ROWS, head), jnp.bfloat16)
        key_slot, value_slot = lax.rem(b, KEY_SLOTS), lax.rem(b, VALUE_SLOTS)
        pieces = range(tiles_in)
        sums, highs, totals, weights = {}, {}, {}, {}

        def score(j):
            q16 = qq[ROWS * j : ROWS * (j + 1)].astype(jnp.bfloat16)
            lhs = jnp.concatenate([jnp.concatenate([q16, zero], 1), jnp.concatenate([zero, q16], 1)], 0)
            s = {}
            for t in pieces:
                rhs = tile_of(kbuf, key_slot, j, t)
                s[t] = lax.dot_general(lhs, rhs, (((1,), (1,)), ((), ())), preferred_element_type=jnp.float32)
                s[t] = jnp.where(own, s[t], -jnp.inf)
            high = jnp.max(functools.reduce(jnp.maximum, s.values()), 1, keepdims=True)
            high = jnp.maximum(high[:ROWS], high[ROWS:])
            both = jnp.concatenate([high, high], 0)
            p = {t: jnp.exp2((s[t] - both) * scale) for t in s}
            total = jnp.sum(sum(p.values()), 1, keepdims=True)
            weights[j] = {t: p[t].astype(jnp.bfloat16) for t in p}
            highs[j], totals[j] = high, total[:ROWS] + total[ROWS:]

        def value(j):
            o = sum(
                jnp.dot(weights[j][t], tile_of(vbuf, value_slot, j, t), preferred_element_type=jnp.float32) for t in pieces
            )
            sums[j] = o[:ROWS, :head] + o[ROWS:, head:]

        ratios = {}

        def settle():
            lane = lax.broadcasted_iota(jnp.int32, (8, head), 1)
            tile = jnp.zeros((8, head), jnp.float32)
            for g in range(tiles):
                h0, h1 = eight(highs, g), eight(highs, g + tiles)
                high = jnp.maximum(h0, h1)
                e0 = jnp.exp2((h0 - high) * scale)
                e1 = jnp.exp2((h1 - high) * scale)
                tile = jnp.where(lane == g, high, tile)
                tile = jnp.where(lane == g + 8, eight(totals, g) * e0 + eight(totals, g + tiles) * e1, tile)
                ratios[g], ratios[g + tiles] = e0, e1
            stat[b] = tile

        for j in range(groups + delay):
            if j < groups:
                score(j)
            if j == groups and between is not None:
                settle()
                between()
            if j >= delay:
                value(j - delay)
        if between is None:
            settle()
        seen = [eight(sums, g) * ratios[g] + eight(sums, g + tiles) * ratios[g + tiles] for g in range(tiles)]
        part[b] = jnp.concatenate(seen, 0).astype(jnp.bfloat16)

    def together(b):
        for x, ref in enumerate((part_in, stat_in)):
            peers = ref.at[pl.ds(0, n - 1), seat(b)]
            pltpu.make_async_copy(peers, peers, recv_sem.at[x, seat(b)]).wait()
        others = [lax.rem(me + i, n) for i in range(1, n)]
        stats = [stat[b]] + [stat_in[i, seat(b)] for i in others]
        high = functools.reduce(jnp.maximum, stats)
        weights = [jnp.exp2((s - high) * scale) for s in stats]
        total = sum(w * pltpu.roll(s, head - 8, 1) for w, s in zip(weights, stats))
        weights = [w / total for w in weights]
        acc = [jnp.zeros((8, head), jnp.float32)] * tiles
        for i in range(n):
            mine = (part_in[others[i - 1], seat(b)] if i else part[b]).astype(jnp.float32)
            for g in range(tiles):
                acc[g] = acc[g] + mine[8 * g : 8 * (g + 1)] * weights[i][:, g : g + 1]
        out[b] = jnp.concatenate(acc, 0).astype(jnp.bfloat16)

    def step(b, _):
        key_copy(b).wait()
        value_copy(b).wait()

        @pl.when(b + 3 < batch)
        def _():
            key_copy(b + 3).start()

        attend(b, DELAY)
        value_copy(b + 2).start()
        give_owner(b)

        @pl.when(b >= LAG)
        def _():
            finish(b - LAG)

        return 0

    def last_step(b, _):
        key_copy(b).wait()

        def between():
            give_all(1, b)
            value_copy(b).wait()

        attend(b, groups, between)
        give_all(0, b)
        finish(b - LAG)
        return 0

    lax.fori_loop(0, owned, step, 0)
    lax.fori_loop(owned, batch, last_step, 0)
    def drain(b, _):
        @pl.when(lax.rem(b, n) == me)
        def _():
            sent = out.at[pl.ds(0, n - 1)]
            pltpu.make_async_copy(sent, sent, spread_sem.at[b]).wait()

        @pl.when(lax.rem(b, n) != me)
        def _():
            for x, ref in enumerate((part, stat)):
                pltpu.make_async_copy(ref.at[b], ref.at[b], give_sem.at[x, b]).wait()
            pltpu.make_async_copy(out.at[b], out.at[b], done_sem.at[b]).wait()

        return 0

    lax.fori_loop(0, owned, drain, 0)
    lax.fori_loop(owned, batch, lambda b, _: (together(b), 0)[1], 0)
    for x, ref in enumerate((part_in, stat_in)):
        sent = ref.at[pl.ds(0, n - 1), pl.ds(0, TAIL)]
        pltpu.make_async_copy(sent, sent, send_sem.at[x]).wait()


def solution(mesh):
    n = mesh.shape["sp"]

    def step(q, k, v):
        batch, heads, head = q.shape
        tokens = k.shape[1]
        groups = 2 * heads // ROWS
        seats = -(-(batch - TAIL) // n) + TAIL
        shape = (batch, tokens // 4, 2, groups, ROWS, head)
        return pl.pallas_call(
            functools.partial(kernel, n),
            out_shape=jax.ShapeDtypeStruct(q.shape, q.dtype),
            in_specs=[pl.BlockSpec(memory_space=pl.ANY)] * 3,
            out_specs=pl.BlockSpec(memory_space=pltpu.VMEM),
            scratch_shapes=[
                pltpu.VMEM((KEY_SLOTS,) + shape[1:], jnp.bfloat16),
                pltpu.VMEM((VALUE_SLOTS,) + shape[1:], jnp.bfloat16),
                pltpu.VMEM(q.shape, jnp.bfloat16),
                pltpu.VMEM(q.shape, jnp.bfloat16),
                pltpu.VMEM((batch, 8, head), jnp.float32),
                pltpu.VMEM((n, seats, heads, head), jnp.bfloat16),
                pltpu.VMEM((n, seats, 8, head), jnp.float32),
                pltpu.SemaphoreType.DMA((KEY_SLOTS,)),
                pltpu.SemaphoreType.DMA((VALUE_SLOTS,)),
                pltpu.SemaphoreType.DMA,
                pltpu.SemaphoreType.DMA((batch,)),
                pltpu.SemaphoreType.DMA((batch,)),
                pltpu.SemaphoreType.DMA((2, batch)),
                pltpu.SemaphoreType.DMA((2,)),
                pltpu.SemaphoreType.DMA((2, seats)),
            ],
            compiler_params=pltpu.CompilerParams(
                collective_id=0, has_side_effects=True, vmem_limit_bytes=40 * 1024 * 1024
            ),
        )(pltpu.with_memory_space_constraint(q, pltpu.HBM), k.reshape(shape), v.reshape(shape))

    return jax.shard_map(
        step,
        mesh=mesh,
        in_specs=(P("dp", None, None), P("dp", "sp", None, None), P("dp", "sp", None, None)),
        out_specs=P("dp", None, None),
        check_vma=False,
    )
```

```python
import functools

import jax
import jax.numpy as jnp
from jax import lax
from jax.experimental import pallas as pl
from jax.experimental.pallas import tpu as pltpu
from jax.sharding import PartitionSpec as P

MESH = pl.DeviceIdType.MESH
LOG2E = 1.4426950408889634
LAG = 2
KEY_SLOTS = 3
VALUE_SLOTS = 3
TAIL = 2
ROWS = 16
TILE = 256
DELAY = 5


def kernel(
    n, q_hbm, k_hbm, v_hbm, out, kbuf, vbuf, qbuf, part, stat, part_in, stat_in,
    ksem, vsem, qsem, done_sem, spread_sem, give_sem, send_sem, recv_sem
):
    batch, half, _, groups, _, head = k_hbm.shape
    heads = q_hbm.shape[1]
    tiles = heads // 8
    me = lax.axis_index("sp")
    dp = lax.axis_index("dp")
    scale = head**-0.5 * LOG2E

    def fetch(hbm, buf, sem, b):
        slot = lax.rem(b, buf.shape[0])
        return pltpu.make_async_copy(hbm.at[b], buf.at[slot], sem.at[slot])

    def key_copy(b):
        return fetch(k_hbm, kbuf, ksem, b)

    def value_copy(b):
        return fetch(v_hbm, vbuf, vsem, b)

    q_copy = pltpu.make_async_copy(q_hbm, qbuf, qsem)
    q_copy.start()
    key_copy(0).start()
    value_copy(0).start()

    barrier = pltpu.get_barrier_semaphore()
    for i in range(1, n):
        pl.semaphore_signal(barrier, inc=1, device_id=(dp, lax.rem(me + i, n)), device_id_type=MESH)
    q_copy.wait()
    key_copy(1).start()
    value_copy(1).start()
    pl.semaphore_wait(barrier, n - 1)

    owned = batch - TAIL
    rounds = -(-owned // n)

    def seat(b):
        return jnp.where(b < owned, b // n, b - owned + rounds)

    def give(x, b, peer, sem):
        ref, dst = ((part, part_in), (stat, stat_in))[x]
        pltpu.make_async_remote_copy(
            src_ref=ref.at[b],
            dst_ref=dst.at[me, seat(b)],
            send_sem=sem,
            recv_sem=recv_sem.at[x, seat(b)],
            device_id=(dp, peer),
            device_id_type=MESH,
        ).start()

    x, y, core = me // 4, me // 2 % 2, me % 2
    far_first = [
        (x + dx) % 2 * 4 + (y + dy) % 2 * 2 + (core + dc) % 2
        for dx, dy, dc in ((1, 1, 0), (1, 1, 1), (1, 0, 0), (0, 1, 0), (1, 0, 1), (0, 1, 1), (0, 0, 1))
    ]

    def give_owner(b):
        @pl.when(lax.rem(b, n) != me)
        def _():
            for x in range(2):
                give(x, b, lax.rem(b, n), give_sem.at[x, b])

    def give_all(b):
        for peer in far_first:
            for x in range(2):
                give(x, b, peer, send_sem.at[x])

    def spread(b):
        for i in range(1, n):
            pltpu.make_async_remote_copy(
                src_ref=out.at[b],
                dst_ref=out.at[b],
                send_sem=spread_sem.at[b],
                recv_sem=done_sem.at[b],
                device_id=(dp, lax.rem(me + i, n)),
                device_id_type=MESH,
            ).start()

    def finish(b):
        @pl.when(lax.rem(b, n) == me)
        def _():
            together(b)
            spread(b)

    tiles_in = half * ROWS // TILE

    def tile_of(buf, slot, j, t):
        step = TILE // ROWS
        rows = [buf[slot, step * t : step * (t + 1), a, j].reshape(TILE, head) for a in range(2)]
        return jnp.concatenate(rows, 1)

    def eight(pieces, g):
        return pieces[8 * g // ROWS][8 * g % ROWS : 8 * g % ROWS + 8]

    def attend(b):
        q32 = qbuf[b].astype(jnp.float32)
        qq = jnp.concatenate([q32, q32], 0)
        row = lax.broadcasted_iota(jnp.int32, (2 * ROWS, TILE), 0) % ROWS
        col = lax.broadcasted_iota(jnp.int32, (2 * ROWS, TILE), 1) % ROWS
        own = row == col
        zero = jnp.zeros((ROWS, head), jnp.bfloat16)
        key_slot, value_slot = lax.rem(b, KEY_SLOTS), lax.rem(b, VALUE_SLOTS)
        pieces = range(tiles_in)
        sums, highs, totals, weights = {}, {}, {}, {}

        def score(j):
            q16 = qq[ROWS * j : ROWS * (j + 1)].astype(jnp.bfloat16)
            lhs = jnp.concatenate([jnp.concatenate([q16, zero], 1), jnp.concatenate([zero, q16], 1)], 0)
            s = {}
            for t in pieces:
                rhs = tile_of(kbuf, key_slot, j, t)
                s[t] = lax.dot_general(lhs, rhs, (((1,), (1,)), ((), ())), preferred_element_type=jnp.float32)
                s[t] = jnp.where(own, s[t], -jnp.inf)
            high = jnp.max(functools.reduce(jnp.maximum, s.values()), 1, keepdims=True)
            high = jnp.maximum(high[:ROWS], high[ROWS:])
            both = jnp.concatenate([high, high], 0)
            p = {t: jnp.exp2((s[t] - both) * scale) for t in s}
            total = jnp.sum(sum(p.values()), 1, keepdims=True)
            weights[j] = {t: p[t].astype(jnp.bfloat16) for t in p}
            highs[j], totals[j] = high, total[:ROWS] + total[ROWS:]

        def value(j):
            o = sum(
                jnp.dot(weights[j][t], tile_of(vbuf, value_slot, j, t), preferred_element_type=jnp.float32) for t in pieces
            )
            sums[j] = o[:ROWS, :head] + o[ROWS:, head:]

        ratios = {}

        def settle():
            lane = lax.broadcasted_iota(jnp.int32, (8, head), 1)
            tile = jnp.zeros((8, head), jnp.float32)
            for g in range(tiles):
                h0, h1 = eight(highs, g), eight(highs, g + tiles)
                high = jnp.maximum(h0, h1)
                e0 = jnp.exp2((h0 - high) * scale)
                e1 = jnp.exp2((h1 - high) * scale)
                tile = jnp.where(lane == g, high, tile)
                tile = jnp.where(lane == g + 8, eight(totals, g) * e0 + eight(totals, g + tiles) * e1, tile)
                ratios[g], ratios[g + tiles] = e0, e1
            stat[b] = tile

        for j in range(groups + DELAY):
            if j < groups:
                score(j)
            if j >= DELAY:
                value(j - DELAY)
        settle()
        seen = [eight(sums, g) * ratios[g] + eight(sums, g + tiles) * ratios[g + tiles] for g in range(tiles)]
        part[b] = jnp.concatenate(seen, 0).astype(jnp.bfloat16)

    def together(b):
        for x, ref in enumerate((part_in, stat_in)):
            peers = ref.at[pl.ds(0, n - 1), seat(b)]
            pltpu.make_async_copy(peers, peers, recv_sem.at[x, seat(b)]).wait()
        others = [lax.rem(me + i, n) for i in range(1, n)]
        stats = [stat[b]] + [stat_in[i, seat(b)] for i in others]
        high = functools.reduce(jnp.maximum, stats)
        weights = [jnp.exp2((s - high) * scale) for s in stats]
        total = sum(w * pltpu.roll(s, head - 8, 1) for w, s in zip(weights, stats))
        weights = [w / total for w in weights]
        acc = [jnp.zeros((8, head), jnp.float32)] * tiles
        for i in range(n):
            mine = (part_in[others[i - 1], seat(b)] if i else part[b]).astype(jnp.float32)
            for g in range(tiles):
                acc[g] = acc[g] + mine[8 * g : 8 * (g + 1)] * weights[i][:, g : g + 1]
        out[b] = jnp.concatenate(acc, 0).astype(jnp.bfloat16)

    def step(b, _):
        key_copy(b).wait()
        value_copy(b).wait()

        @pl.when(b + 2 < batch)
        def _():
            key_copy(b + 2).start()
            value_copy(b + 2).start()

        attend(b)

        @pl.when(b < owned)
        def _():
            give_owner(b)

        @pl.when(b >= owned)
        def _():
            give_all(b)

        @pl.when(b >= LAG)
        def _():
            finish(b - LAG)

        return 0

    lax.fori_loop(0, batch, step, 0)
    def drain(b, _):
        @pl.when(lax.rem(b, n) == me)
        def _():
            sent = out.at[pl.ds(0, n - 1)]
            pltpu.make_async_copy(sent, sent, spread_sem.at[b]).wait()

        @pl.when(lax.rem(b, n) != me)
        def _():
            for x, ref in enumerate((part, stat)):
                pltpu.make_async_copy(ref.at[b], ref.at[b], give_sem.at[x, b]).wait()
            pltpu.make_async_copy(out.at[b], out.at[b], done_sem.at[b]).wait()

        return 0

    lax.fori_loop(0, owned, drain, 0)
    lax.fori_loop(owned, batch, lambda b, _: (together(b), 0)[1], 0)
    for x, ref in enumerate((part_in, stat_in)):
        sent = ref.at[pl.ds(0, n - 1), pl.ds(0, TAIL)]
        pltpu.make_async_copy(sent, sent, send_sem.at[x]).wait()


def solution(mesh):
    n = mesh.shape["sp"]

    def step(q, k, v):
        batch, heads, head = q.shape
        tokens = k.shape[1]
        groups = 2 * heads // ROWS
        seats = -(-(batch - TAIL) // n) + TAIL
        shape = (batch, tokens // 4, 2, groups, ROWS, head)
        return pl.pallas_call(
            functools.partial(kernel, n),
            out_shape=jax.ShapeDtypeStruct(q.shape, q.dtype),
            in_specs=[pl.BlockSpec(memory_space=pl.ANY)] * 3,
            out_specs=pl.BlockSpec(memory_space=pltpu.VMEM),
            scratch_shapes=[
                pltpu.VMEM((KEY_SLOTS,) + shape[1:], jnp.bfloat16),
                pltpu.VMEM((VALUE_SLOTS,) + shape[1:], jnp.bfloat16),
                pltpu.VMEM(q.shape, jnp.bfloat16),
                pltpu.VMEM(q.shape, jnp.bfloat16),
                pltpu.VMEM((batch, 8, head), jnp.float32),
                pltpu.VMEM((n, seats, heads, head), jnp.bfloat16),
                pltpu.VMEM((n, seats, 8, head), jnp.float32),
                pltpu.SemaphoreType.DMA((KEY_SLOTS,)),
                pltpu.SemaphoreType.DMA((VALUE_SLOTS,)),
                pltpu.SemaphoreType.DMA,
                pltpu.SemaphoreType.DMA((batch,)),
                pltpu.SemaphoreType.DMA((batch,)),
                pltpu.SemaphoreType.DMA((2, batch)),
                pltpu.SemaphoreType.DMA((2,)),
                pltpu.SemaphoreType.DMA((2, seats)),
            ],
            compiler_params=pltpu.CompilerParams(
                collective_id=0, has_side_effects=True, vmem_limit_bytes=40 * 1024 * 1024
            ),
        )(pltpu.with_memory_space_constraint(q, pltpu.HBM), k.reshape(shape), v.reshape(shape))

    return jax.shard_map(
        step,
        mesh=mesh,
        in_specs=(P("dp", None, None), P("dp", "sp", None, None), P("dp", "sp", None, None)),
        out_specs=P("dp", None, None),
        check_vma=False,
    )
```

```python
import functools

import jax
import jax.numpy as jnp
from jax import lax
from jax.experimental import pallas as pl
from jax.experimental.pallas import tpu as pltpu
from jax.sharding import PartitionSpec as P

MESH = pl.DeviceIdType.MESH
LOG2E = 1.4426950408889634
LAG = 2
LEAD = 2
SLOTS = 3
TAIL = 4
ROWS = 16
TILE = 256
DELAY = 7


def kernel(
    n, q_hbm, k_hbm, v_hbm, out, kbuf, vbuf, qbuf, w0, w1, w2, r0, r1, r2, part, stat, part_in, stat_in,
    ksem, vsem, qsem, done_sem, spread_sem, give_sem, send_sem, recv_sem
):
    batch, half, _, groups, _, head = k_hbm.shape
    heads = q_hbm.shape[1]
    tiles = heads // 8
    me = lax.axis_index("sp")
    dp = lax.axis_index("dp")
    scale = head**-0.5 * LOG2E

    def fetch(hbm, buf, sem, b):
        slot = lax.rem(b, buf.shape[0])
        return pltpu.make_async_copy(hbm.at[b], buf.at[slot], sem.at[slot])

    def key_copy(b):
        return fetch(k_hbm, kbuf, ksem, b)

    def value_copy(b):
        return fetch(v_hbm, vbuf, vsem, b)

    q_copy = pltpu.make_async_copy(q_hbm, qbuf, qsem)
    q_copy.start()
    for b in range(SLOTS):
        key_copy(b).start()

    barrier = pltpu.get_barrier_semaphore()
    for i in range(1, n):
        pl.semaphore_signal(barrier, inc=1, device_id=(dp, lax.rem(me + i, n)), device_id_type=MESH)
    q_copy.wait()
    pl.semaphore_wait(barrier, n - 1)

    owned = batch - TAIL
    rounds = -(-owned // n)

    def seat(b):
        return jnp.where(b < owned, b // n, b - owned + rounds)

    def give(x, b, peer, sem):
        ref, dst = ((part, part_in), (stat, stat_in))[x]
        pltpu.make_async_remote_copy(
            src_ref=ref.at[b],
            dst_ref=dst.at[me, seat(b)],
            send_sem=sem,
            recv_sem=recv_sem.at[x, seat(b)],
            device_id=(dp, peer),
            device_id_type=MESH,
        ).start()

    x, y, core = me // 4, me // 2 % 2, me % 2
    far_first = [
        (x + dx) % 2 * 4 + (y + dy) % 2 * 2 + (core + dc) % 2
        for dx, dy, dc in ((1, 1, 0), (1, 1, 1), (1, 0, 0), (0, 1, 0), (1, 0, 1), (0, 1, 1), (0, 0, 1))
    ]

    def give_owner(x, b):
        @pl.when(lax.rem(b, n) != me)
        def _():
            give(x, b, lax.rem(b, n), give_sem.at[x, b])

    def give_all(x, b):
        for peer in far_first:
            give(x, b, peer, send_sem.at[x])

    def spread(b):
        for i in range(1, n):
            pltpu.make_async_remote_copy(
                src_ref=out.at[b],
                dst_ref=out.at[b],
                send_sem=spread_sem.at[b],
                recv_sem=done_sem.at[b],
                device_id=(dp, lax.rem(me + i, n)),
                device_id_type=MESH,
            ).start()

    def finish(b):
        @pl.when(lax.rem(b, n) == me)
        def _():
            together(b)
            spread(b)

    weight_bufs, ratio_bufs = (w0, w1, w2), (r0, r1, r2)
    tiles_in = half * ROWS // TILE

    def tile_of(buf, slot, j, t):
        step = TILE // ROWS
        rows = [buf[slot, step * t : step * (t + 1), a, j].reshape(TILE, head) for a in range(2)]
        return jnp.concatenate(rows, 1)

    def eight(pieces, g):
        return pieces[8 * g // ROWS][8 * g % ROWS : 8 * g % ROWS + 8]

    def stage(b, x, scoring, summing):
        key_slot, value_slot = lax.rem(b, SLOTS), lax.rem(b - LEAD + SLOTS, SLOTS)
        wbuf, ebuf = weight_bufs[x], ratio_bufs[x]
        old_wbuf, old_ebuf = weight_bufs[(x + 1) % SLOTS], ratio_bufs[(x + 1) % SLOTS]
        pieces = range(tiles_in)
        sums, highs, totals = {}, {}, {}

        def score(j):
            q16 = qq[ROWS * j : ROWS * (j + 1)].astype(jnp.bfloat16)
            lhs = jnp.concatenate([jnp.concatenate([q16, zero], 1), jnp.concatenate([zero, q16], 1)], 0)
            s = {}
            for t in pieces:
                rhs = tile_of(kbuf, key_slot, j, t)
                s[t] = lax.dot_general(lhs, rhs, (((1,), (1,)), ((), ())), preferred_element_type=jnp.float32)
                s[t] = jnp.where(own, s[t], -jnp.inf)
            high = jnp.max(functools.reduce(jnp.maximum, s.values()), 1, keepdims=True)
            high = jnp.maximum(high[:ROWS], high[ROWS:])
            both = jnp.concatenate([high, high], 0)
            p = {t: jnp.exp2((s[t] - both) * scale) for t in s}
            total = jnp.sum(sum(p.values()), 1, keepdims=True)
            for t in p:
                wbuf[j, t] = p[t].astype(jnp.bfloat16)
            highs[j], totals[j] = high, total[:ROWS] + total[ROWS:]

        def value(j):
            o = sum(
                jnp.dot(old_wbuf[j, t], tile_of(vbuf, value_slot, j, t), preferred_element_type=jnp.float32)
                for t in pieces
            )
            sums[j] = o[:ROWS, :head] + o[ROWS:, head:]

        if scoring:
            q32 = qbuf[b].astype(jnp.float32)
            qq = jnp.concatenate([q32, q32], 0)
            row = lax.broadcasted_iota(jnp.int32, (2 * ROWS, TILE), 0) % ROWS
            col = lax.broadcasted_iota(jnp.int32, (2 * ROWS, TILE), 1) % ROWS
            own = row == col
            zero = jnp.zeros((ROWS, head), jnp.bfloat16)
        for j in range(groups + DELAY):
            if scoring and j < groups:
                score(j)
            if summing and j >= DELAY:
                value(j - DELAY)
        if scoring:
            lane = lax.broadcasted_iota(jnp.int32, (8, head), 1)
            tile = jnp.zeros((8, head), jnp.float32)
            for g in range(tiles):
                h0, h1 = eight(highs, g), eight(highs, g + tiles)
                high = jnp.maximum(h0, h1)
                e0 = jnp.exp2((h0 - high) * scale)
                e1 = jnp.exp2((h1 - high) * scale)
                ebuf[g] = jnp.broadcast_to(e0, (8, head))
                ebuf[g + tiles] = jnp.broadcast_to(e1, (8, head))
                tile = jnp.where(lane == g, high, tile)
                tile = jnp.where(lane == g + 8, eight(totals, g) * e0 + eight(totals, g + tiles) * e1, tile)
            stat[b] = tile
        if summing:
            seen = [eight(sums, g) * old_ebuf[g] + eight(sums, g + tiles) * old_ebuf[g + tiles] for g in range(tiles)]
            part[b - LEAD] = jnp.concatenate(seen, 0).astype(jnp.bfloat16)

    def together(b):
        for x, ref in enumerate((part_in, stat_in)):
            peers = ref.at[pl.ds(0, n - 1), seat(b)]
            pltpu.make_async_copy(peers, peers, recv_sem.at[x, seat(b)]).wait()
        others = [lax.rem(me + i, n) for i in range(1, n)]
        stats = [stat[b]] + [stat_in[i, seat(b)] for i in others]
        high = functools.reduce(jnp.maximum, stats)
        weights = [jnp.exp2((s - high) * scale) for s in stats]
        total = sum(w * pltpu.roll(s, head - 8, 1) for w, s in zip(weights, stats))
        weights = [w / total for w in weights]
        acc = [jnp.zeros((8, head), jnp.float32)] * tiles
        for i in range(n):
            mine = (part_in[others[i - 1], seat(b)] if i else part[b]).astype(jnp.float32)
            for g in range(tiles):
                acc[g] = acc[g] + mine[8 * g : 8 * (g + 1)] * weights[i][:, g : g + 1]
        out[b] = jnp.concatenate(acc, 0).astype(jnp.bfloat16)

    def share(x, b):
        @pl.when(b < owned)
        def _():
            give_owner(x, b)

        @pl.when(b >= owned)
        def _():
            give_all(x, b)

    def step(b, x):
        key_copy(b).wait()
        value_copy(b - LEAD).wait()

        @pl.when(b + 2 < batch)
        def _():
            key_copy(b + 2).start()

        value_copy(b).start()
        stage(b, x, True, True)
        share(0, b - LEAD)
        share(1, b)

        @pl.when(b >= LEAD + LAG)
        def _():
            finish(b - LEAD - LAG)

    def steps(i, _):
        for u in range(SLOTS):
            step(LEAD + SLOTS * i + u, (LEAD + u) % SLOTS)
        return 0

    for b in range(LEAD):
        key_copy(b).wait()
        if b:
            key_copy(b + 2).start()
        value_copy(b).start()
        stage(b, b, True, False)
        give_owner(1, b)
    lax.fori_loop(0, (batch - LEAD) // SLOTS, steps, 0)
    for b in range(batch, batch + LEAD):
        value_copy(b - LEAD).wait()
        stage(b, b % SLOTS, False, True)
        give_all(0, b - LEAD)
    def drain(b, _):
        @pl.when(lax.rem(b, n) == me)
        def _():
            sent = out.at[pl.ds(0, n - 1)]
            pltpu.make_async_copy(sent, sent, spread_sem.at[b]).wait()

        @pl.when(lax.rem(b, n) != me)
        def _():
            for x, ref in enumerate((part, stat)):
                pltpu.make_async_copy(ref.at[b], ref.at[b], give_sem.at[x, b]).wait()
            pltpu.make_async_copy(out.at[b], out.at[b], done_sem.at[b]).wait()

        return 0

    lax.fori_loop(0, owned, drain, 0)
    lax.fori_loop(owned, batch, lambda b, _: (together(b), 0)[1], 0)
    for x, ref in enumerate((part_in, stat_in)):
        sent = ref.at[pl.ds(0, n - 1), pl.ds(0, TAIL)]
        pltpu.make_async_copy(sent, sent, send_sem.at[x]).wait()


def solution(mesh):
    n = mesh.shape["sp"]

    def step(q, k, v):
        batch, heads, head = q.shape
        tokens = k.shape[1]
        groups = 2 * heads // ROWS
        seats = -(-(batch - TAIL) // n) + TAIL
        shape = (batch, tokens // 4, 2, groups, ROWS, head)
        return pl.pallas_call(
            functools.partial(kernel, n),
            out_shape=jax.ShapeDtypeStruct(q.shape, q.dtype),
            in_specs=[pl.BlockSpec(memory_space=pl.ANY)] * 3,
            out_specs=pl.BlockSpec(memory_space=pltpu.VMEM),
            scratch_shapes=[
                pltpu.VMEM((SLOTS,) + shape[1:], jnp.bfloat16),
                pltpu.VMEM((SLOTS,) + shape[1:], jnp.bfloat16),
                pltpu.VMEM(q.shape, jnp.bfloat16),
                *[pltpu.VMEM((groups, tokens // 4 * ROWS // TILE, 2 * ROWS, TILE), jnp.bfloat16)] * SLOTS,
                *[pltpu.VMEM((groups * ROWS // 8, 8, head), jnp.float32)] * SLOTS,
                pltpu.VMEM(q.shape, jnp.bfloat16),
                pltpu.VMEM((batch, 8, head), jnp.float32),
                pltpu.VMEM((n, seats, heads, head), jnp.bfloat16),
                pltpu.VMEM((n, seats, 8, head), jnp.float32),
                pltpu.SemaphoreType.DMA((SLOTS,)),
                pltpu.SemaphoreType.DMA((SLOTS,)),
                pltpu.SemaphoreType.DMA,
                pltpu.SemaphoreType.DMA((batch,)),
                pltpu.SemaphoreType.DMA((batch,)),
                pltpu.SemaphoreType.DMA((2, batch)),
                pltpu.SemaphoreType.DMA((2,)),
                pltpu.SemaphoreType.DMA((2, seats)),
            ],
            compiler_params=pltpu.CompilerParams(
                collective_id=0, has_side_effects=True, vmem_limit_bytes=40 * 1024 * 1024
            ),
        )(pltpu.with_memory_space_constraint(q, pltpu.HBM), k.reshape(shape), v.reshape(shape))

    return jax.shard_map(
        step,
        mesh=mesh,
        in_specs=(P("dp", None, None), P("dp", "sp", None, None), P("dp", "sp", None, None)),
        out_specs=P("dp", None, None),
        check_vma=False,
    )
```
